32 devices in a mesh: out: 8 (over z, x), inp: 4 (over y, core).
Axes of the slice: x: 2, y: 2, z: 4, core: 2. Of those that a mesh axis runs over, the one named last changes fastest.
Arguments:
- tensor: bfloat16 [1024, 1024, 1024], P('out', 'inp'), may hold values from -0.005859375 to 0.005859375
- state: bfloat16 [768, 1024], P('out'), may hold values from -6 to 6
Outputs:
- collision: bfloat16 [768, 1024], P('inp', 'out')
The draws below stay inside these ranges and needn't reach their ends.
All inputs are finite; a program needn't handle non-finite values.
Results may differ from the reference program's by a relative error of at most 0.001.
Values may be sent and summed in bfloat16 or wider, within the bound.
A program may use at most 128 MiB of HBM per device.

```python
import jax
import jax.numpy as jnp
from jax import lax

K = 1024
CELLS = 768


def shard_levels(key, shape, split, least, high):
    loudness, own = 1.0, jax.random.fold_in(key, 6)
    for dim, shards_of in split:
        steps = jnp.exp(jax.random.uniform(jax.random.fold_in(own, dim), (shards_of,), jnp.float32, least / len(split), high / len(split)))
        loudness = loudness * jnp.repeat(steps, shape[dim] // shards_of).reshape([-1 if axis == dim else 1 for axis in range(len(shape))])
    return loudness


def centred(own_key, extent, scale, most, shards=(), kind=jnp.bfloat16):
    drawn = jax.random.normal(own_key, extent, jnp.float32) * scale
    if len(shards) > 0:
        drawn = shard_levels(own_key, extent, shards, -0.22, 0.18) * drawn
    return jnp.clip(drawn, min=-most, max=most).astype(kind)


def setup_inputs(seed: int = 0) -> dict:
    key_list = jax.random.split(jax.random.key(seed), 3)
    return {
        "tensor": centred(key_list[0], (K, K, K), (K * K) ** -0.5, 0.005859375, ((0, 8), (1, 4))),
        "state": centred(key_list[1], (CELLS, K), 1.0, 6.0, ((0, 8),)),
    }


def reference(tensor, state):
    blocks = tensor.reshape(K // 16, 16, K, K)
    state_wide = state.astype(jnp.float32)

    def one_block(slab):
        flat = slab.reshape(16 * K, K)
        inner = lax.dot_general(state, flat, (((1,), (1,)), ((), ())), preferred_element_type=jnp.float32)
        inner = inner.reshape(state.shape[0], 16, K)
        return jnp.sum(inner * state_wide[:, None, :], axis=2)

    parts = lax.map(one_block, blocks)
    result = jnp.transpose(parts, (1, 0, 2)).reshape(state.shape[0], K)
    return result.astype(jnp.bfloat16)
```

```python
import functools

import jax
import jax.numpy as jnp
from jax import lax
from jax.experimental import pallas as pl
from jax.experimental.pallas import tpu as pltpu
from jax.sharding import PartitionSpec as P

MESH = pl.DeviceIdType.MESH
GROUP = 16
SLOTS = 5


def flip(value, bits):
    for bit in (1 << n for n in range(bits.bit_length())):
        if bits & bit:
            value = value + bit * (1 - 2 * ((value // bit) % 2))
    return value


def kernel(nx, n_out, n_inp, tensor, state, out, gathered, turned, chosen, slab, parts, landed,
           own_sem, z_sems, x_sems, core_sems, t_sems, s_sems, r_sems):
    rows_out, rows_inp, width = tensor.shape
    cells_own = state.shape[0]
    cells = n_out * cells_own
    nz = n_out // nx
    per_owner = n_out // n_inp
    group = slab.shape[1]
    blocks = rows_out // group
    slots = slab.shape[0]
    lanes = 256 if cells % 256 == 0 else cells
    halves = 2
    half_width = width // halves
    early = -(-lanes // cells_own)

    me_o = lax.axis_index("out")
    me_p = lax.axis_index("inp")
    z, x = me_o // nx, me_o % nx
    half = me_p % halves
    partner = me_p + 1 - 2 * half
    cols = pl.ds(pl.multiple_of(half * half_width, 128), half_width)

    def fetch(b, slot):
        return pltpu.make_async_copy(
            tensor.at[pl.ds(b * group, group)], slab.at[slot], t_sems.at[slot])

    own_copy = pltpu.make_async_copy(state, gathered.at[pl.ds(0, cells_own)], own_sem)
    own_copy.start()
    for b in range(slots):
        fetch(b, b).start()

    def out_of(d, e):
        return flip(z, d) * nx + flip(x, e)

    barrier = pltpu.get_barrier_semaphore()
    near = [(out_of(d, 0), me_p) for d in range(1, nz)]
    near += [(out_of(0, e), me_p) for e in range(1, nx)]
    near += [(me_o, lax.rem(me_p + q, n_inp)) for q in range(1, n_inp)]
    for device in near:
        pl.semaphore_signal(barrier, inc=1, device_id=device, device_id_type=MESH)
    pl.semaphore_wait(barrier, len(near))

    def remote(src, dst, send, recv, device):
        return pltpu.make_async_remote_copy(
            src_ref=src, dst_ref=dst, send_sem=send, recv_sem=recv,
            device_id=device, device_id_type=MESH)

    def shard(d, e):
        return gathered.at[pl.ds((d * nx + e) * cells_own, cells_own), cols]

    def z_copy(d):
        return remote(state.at[:, cols], shard(d, 0), z_sems.at[0, d], z_sems.at[1, d],
                      (out_of(d, 0), me_p))

    def x_copy(e, d):
        return remote(state.at[:, cols] if d == 0 else shard(d, 0), shard(d, e),
                      x_sems.at[0, e, d], x_sems.at[1, e, d], (out_of(0, e), me_p))

    def core_copy(e, d):
        return remote(shard(d, e), shard(d, e), core_sems.at[0, e, d], core_sems.at[1, e, d],
                      (me_o, partner))

    def relay_x(d):
        for e in range(1, nx):
            x_copy(e, d).wait_recv()
            core_copy(e, d).start()

    def relay_z(d):
        z_copy(d).wait_recv()
        for e in range(1, nx):
            x_copy(e, d).start()
        core_copy(0, d).start()

    for e in range(1, nx):
        x_copy(e, 0).start()
    for d in range(1, nz):
        z_copy(d).start()
    own_copy.wait()
    relay_x(0)
    relay_z(1)
    order = [(d, e) for d in range(nz) for e in range(nx)]
    for d, e in order[1:early]:
        core_copy(e, d).wait_recv()

    first = pl.multiple_of(me_p * rows_inp, rows_inp)

    def turn(start, stop):
        for j in range(0, width, 128):
            turned[j:j + 128, start:stop] = gathered[start:stop, j:j + 128].T
        chosen[:, start:stop] = turned[pl.ds(first, rows_inp), start:stop].astype(jnp.float32)

    def send_part(b, q):
        owner = lax.rem(me_p + q, n_inp)
        rows = pl.ds(pl.multiple_of(b * group, group), group)
        return remote(parts.at[pl.ds(owner * per_owner, per_owner), rows],
                      landed.at[q - 1, :, rows],
                      s_sems.at[q - 1], r_sems.at[q - 1], (me_o, owner))

    def products(b, slot, start, stop):
        pieces = []
        for n in range(start, stop, lanes):
            sums = []
            for k in range(group):
                inner = jnp.dot(slab[slot, k], turned[:, n:n + lanes],
                                preferred_element_type=jnp.float32)
                sums.append(jnp.sum(inner * chosen[:, n:n + lanes], axis=0, keepdims=True))
            pieces.append(jnp.concatenate(sums, axis=0))
        total = jnp.concatenate(pieces, axis=1)
        rows = pl.ds(pl.multiple_of(b * group, group), group)
        for s, (d, e) in enumerate(order):
            low, high = max(start, s * cells_own), min(stop, (s + 1) * cells_own)
            if low < high:
                parts[out_of(d, e), rows, low - s * cells_own:high - s * cells_own] = (
                    total[:, low - start:high - start])

    def finish(b, slot):
        for q in range(1, n_inp):
            send_part(b, q).start()

        @pl.when(b + slots < blocks)
        def _():
            fetch(b + slots, slot).start()

    turn(0, lanes)

    def lead(b, carry):
        for d in range(2, nz + 1):
            @pl.when(b == min((d - 1) * slots // max(nz - 1, 1), slots - 1))
            def _():
                if d < nz:
                    relay_z(d)
                relay_x(d - 1)
        fetch(b, b).wait()
        products(b, b, 0, lanes)
        return carry

    lax.fori_loop(0, slots, lead, 0)
    for d, e in order[early:]:
        core_copy(e, d).wait_recv()
    if lanes < cells:
        turn(lanes, cells)

    def follow(b, carry):
        if lanes < cells:
            products(b, b, lanes, cells)
        finish(b, b)
        return carry

    lax.fori_loop(0, slots, follow, 0)

    def whole(b, carry):
        slot = lax.rem(b, slots)
        fetch(b, slot).wait()
        products(b, slot, 0, cells)
        finish(b, slot)
        return carry

    if slots < blocks:
        lax.fori_loop(slots, blocks, whole, 0)

    everything = [remote(parts.at[pl.ds(0, per_owner)], landed.at[q - 1], s_sems.at[q - 1],
                         r_sems.at[q - 1], (me_o, lax.rem(me_p + q, n_inp))) for q in range(1, n_inp)]
    for d in range(1, nz):
        z_copy(d).wait_send()
    for d, e in order:
        if e > 0:
            x_copy(e, d).wait_send()
        if (d, e) != (0, 0):
            core_copy(e, d).wait_send()
    for copy in everything:
        copy.wait_recv()
    for s in range(per_owner):
        total = parts[me_p * per_owner + s]
        for q in range(1, n_inp):
            total = total + landed[q - 1, s]
        out[s * cells_own:(s + 1) * cells_own, :] = total.T[0:cells_own, :].astype(out.dtype)
    for copy in everything:
        copy.wait_send()


def solution(mesh):
    n_out, n_inp = mesh.shape["out"], mesh.shape["inp"]
    nx = len({device.coords[0] for device in mesh.devices[:, 0]})

    def local(tensor, state):
        rows_out, rows_inp, width = tensor.shape
        cells_own = state.shape[0]
        cells = n_out * cells_own
        per_owner = n_out // n_inp
        padded = -(-cells_own // 128) * 128
        nz = n_out // nx
        group = min(GROUP, rows_out)
        slots = min(SLOTS, rows_out // group)
        return pl.pallas_call(
            functools.partial(kernel, nx, n_out, n_inp),
            out_shape=pltpu.VMEM((cells // n_inp, rows_out), jnp.bfloat16),
            in_specs=[pl.BlockSpec(memory_space=pl.ANY), pl.BlockSpec(memory_space=pl.ANY)],
            out_specs=pl.BlockSpec(memory_space=pltpu.VMEM),
            scratch_shapes=[
                pltpu.VMEM((cells, width), jnp.bfloat16),
                pltpu.VMEM((width, cells), jnp.bfloat16),
                pltpu.VMEM((rows_inp, cells), jnp.float32),
                pltpu.VMEM((slots, group, rows_inp, width), jnp.bfloat16),
                pltpu.VMEM((n_out, rows_out, padded), jnp.float32),
                pltpu.VMEM((n_inp - 1, per_owner, rows_out, padded), jnp.float32),
                pltpu.SemaphoreType.DMA,
                pltpu.SemaphoreType.DMA((2, nz)),
                pltpu.SemaphoreType.DMA((2, nx, nz)),
                pltpu.SemaphoreType.DMA((2, nx, nz)),
                pltpu.SemaphoreType.DMA((slots,)),
                pltpu.SemaphoreType.DMA((n_inp - 1,)),
                pltpu.SemaphoreType.DMA((n_inp - 1,)),
            ],
            compiler_params=pltpu.CompilerParams(
                collective_id=0, has_side_effects=True, vmem_limit_bytes=60 * 2**20),
            name="collide",
        )(tensor, state)

    return jax.shard_map(
        local, mesh=mesh, in_specs=(P("out", "inp", None), P("out", None)),
        out_specs=P("inp", "out"), check_vma=False)
```

```python
import functools

import jax
import jax.numpy as jnp
from jax import lax
from jax.experimental import pallas as pl
from jax.experimental.pallas import tpu as pltpu
from jax.sharding import PartitionSpec as P

MESH = pl.DeviceIdType.MESH
GROUP = 16
SLOTS = 6
LAST = 2
OWN = 2
NEAR = 3
HOOKS = (10, 12, 19, 36, 38, 62)
ROWS = (((1,), (1,)), ((), ()))


def flip(value, bits):
    for bit in (1 << n for n in range(bits.bit_length())):
        if bits & bit:
            value = value + bit * (1 - 2 * ((value // bit) % 2))
    return value


def differ(a, b, size):
    total = 0
    for bit in (1 << n for n in range((size - 1).bit_length())):
        total = total + bit * ((a // bit + b // bit) % 2)
    return total


def kernel(nx, n_out, n_inp, tensor, state, out, gathered, chosen, slab, parts, landed,
           own_sem, z_sems, x_sems, core_sems, t_sems, s_sems, r_sems):
    rows_out, rows_inp, width = tensor.shape
    cells_own = state.shape[0]
    cells = n_out * cells_own
    nz = n_out // nx
    per_owner = n_out // n_inp
    slots, group = slab.shape[0], slab.shape[1]
    blocks = rows_out // group
    own = min(OWN, slots - 1)
    near = min(NEAR, n_out)
    halves = 2
    half_width = width // halves

    me_o = lax.axis_index("out")
    me_p = lax.axis_index("inp")
    z, x = me_o // nx, me_o % nx
    half = me_p % halves
    partner = me_p + 1 - 2 * half
    cols = pl.ds(pl.multiple_of(half * half_width, 128), half_width)

    def fetch(b, slot):
        return pltpu.make_async_copy(
            tensor.at[pl.ds(b * group, group)], slab.at[slot], t_sems.at[slot])

    own_copy = pltpu.make_async_copy(state, gathered.at[pl.ds(0, cells_own)], own_sem)
    own_copy.start()
    for b in range(min(2, slots)):
        fetch(b, b).start()

    def out_of(d, e):
        return flip(z, d) * nx + flip(x, e)

    barrier = pltpu.get_barrier_semaphore()
    peers = [(out_of(d, 0), me_p) for d in range(1, nz)]
    peers += [(out_of(0, e), me_p) for e in range(1, nx)]
    peers += [(me_o, lax.rem(me_p + q, n_inp)) for q in range(1, n_inp)]
    for device in peers:
        pl.semaphore_signal(barrier, inc=1, device_id=device, device_id_type=MESH)

    def remote(src, dst, send, recv, device):
        return pltpu.make_async_remote_copy(
            src_ref=src, dst_ref=dst, send_sem=send, recv_sem=recv,
            device_id=device, device_id_type=MESH)

    def shard(d, e):
        return gathered.at[pl.ds((d * nx + e) * cells_own, cells_own), cols]

    def z_copy(d):
        return remote(state.at[:, cols], shard(d, 0), z_sems.at[0, d], z_sems.at[1, d],
                      (out_of(d, 0), me_p))

    def x_copy(e, d):
        return remote(state.at[:, cols] if d == 0 else shard(d, 0), shard(d, e),
                      x_sems.at[0, e, d], x_sems.at[1, e, d], (out_of(0, e), me_p))

    def core_copy(e, d):
        return remote(shard(d, e), shard(d, e), core_sems.at[0, e, d], core_sems.at[1, e, d],
                      (me_o, partner))

    def relay_x(d):
        for e in range(1, nx):
            x_copy(e, d).wait_recv()
            core_copy(e, d).start()

    def relay_z(d):
        z_copy(d).wait_recv()
        for e in range(1, nx):
            x_copy(e, d).start()
        core_copy(0, d).start()

    wide = max(rows_inp, 128)
    first = pl.multiple_of(me_p * rows_inp // wide * wide, wide)

    def choose(start, stop):
        block = gathered[start:stop, pl.ds(first, wide)].astype(jnp.float32)
        piece = block[:, 0:rows_inp]
        for n in range(1, wide // rows_inp):
            piece = jnp.where(me_p % (wide // rows_inp) == n,
                              block[:, n * rows_inp:(n + 1) * rows_inp], piece)
        chosen[start:stop, :] = piece

    def visit(b, slot, start, size, hooks=()):
        rows = pl.ds(start, size)
        lane = lax.broadcasted_iota(jnp.int32, (size, rows_out), 1)
        kept = parts[rows, :]
        for k in range(group):
            for at, act in hooks:
                if at * group // 16 == k:
                    act()
            inner = lax.dot_general(gathered[rows, :], slab[slot, k], ROWS,
                                    preferred_element_type=jnp.float32)
            sums = jnp.sum(inner * chosen[rows, :], axis=1, keepdims=True)
            kept = jnp.where(lane == b * group + k, sums, kept)
        parts[rows, :] = kept

    parts[...] = jnp.zeros_like(parts)
    own_copy.wait()
    choose(0, cells_own)
    pl.semaphore_wait(barrier, len(peers))
    for e in range(1, nx):
        x_copy(e, 0).start()
    for d in range(1, nz):
        z_copy(d).start()

    hooks = [[] for _ in range(slots)]

    def hook(b, at, act):
        hooks[min(b, slots - 1)].append((at, act))

    hook(own - 1, HOOKS[0], lambda: (relay_x(0), relay_z(1)))
    for d in range(2, nz):
        place = HOOKS[min(2 * d - 3, 3)]
        hook(own + place // 16, place % 16, lambda d=d: relay_z(d))
        place = HOOKS[min(2 * d - 2, 4)]
        hook(own + place // 16, place % 16, lambda d=d: relay_x(d - 1))
    hook(own + HOOKS[5] // 16, HOOKS[5] % 16, lambda: relay_x(nz - 1))

    order = [(d, e) for d in range(nz) for e in range(nx)]
    for b in range(slots):
        if b == own:
            for d, e in order[1:near]:
                core_copy(e, d).wait_recv()
            choose(cells_own, near * cells_own)
        fetch(b, b).wait()
        if b + 2 < slots:
            fetch(b + 2, b + 2).start()
        visit(b, b, 0, (1 if b < own else near) * cells_own, hooks[b])
    for d, e in order[near:]:
        core_copy(e, d).wait_recv()
    choose(near * cells_own, cells)

    def refill(b):
        @pl.when(b + slots < blocks)
        def _():
            fetch(b + slots, b).start()

    def most(b, carry):
        visit(b, b, cells_own, cells - cells_own)
        refill(b)
        return carry

    lax.fori_loop(0, own, most, 0)

    def rest(b, carry):
        visit(b, b, near * cells_own, cells - near * cells_own)
        refill(b)
        return carry

    lax.fori_loop(own, slots, rest, 0)

    count = n_out // 2
    span = count * cells_own
    mine = 1 - differ(z // max(nz // 2, 1), me_p // max(n_inp // 2, 1), 2)
    last = blocks - slots

    def sends(side, act):
        for s in range(count):
            zone = flip(z, s // nx)
            zone = zone + side * (nz // 2) * (1 - 2 * ((zone // (nz // 2)) % 2))
            target = zone * nx + flip(x, s % nx)
            owner, place = target // per_owner, target % per_owner

            @pl.when(owner != me_p)
            def _():
                q = lax.rem(owner - me_p + n_inp, n_inp)
                act(remote(
                    parts.at[pl.ds(pl.multiple_of(side * span, 32) + s * cells_own, cells_own)],
                    landed.at[q - 1, place], s_sems.at[q - 1, place], r_sems.at[q - 1, place],
                    (me_o, owner)))

    def finish(t, carry):
        side = differ(t // last, mine, 2)
        b = slots + t % last

        @pl.when(t < last)
        def _():
            fetch(b, b - slots).wait()

        @pl.when(t == last)
        def _():
            sends(mine, lambda copy: copy.start())

        visit(b, b - slots, pl.multiple_of(side * span, 32), span)
        return carry

    lax.fori_loop(0, 2 * last, finish, 0)
    sends(1 - mine, lambda copy: copy.start())

    for d in range(1, nz):
        z_copy(d).wait_send()
    for d, e in order:
        if e > 0:
            x_copy(e, d).wait_send()
        if (d, e) != (0, 0):
            core_copy(e, d).wait_send()
    for s in range(per_owner):
        target = me_p * per_owner + s
        slot = differ(z, target // nx, nz) * nx + differ(x, target % nx, nx)
        total = parts[pl.ds(pl.multiple_of(slot * cells_own, cells_own), cells_own), :]
        for q in range(1, n_inp):
            remote(landed.at[q - 1, s], landed.at[q - 1, s], s_sems.at[q - 1, s],
                   r_sems.at[q - 1, s], (me_o, partner)).wait_recv()
            total = total + landed[q - 1, s]
        out[s * cells_own:(s + 1) * cells_own, :] = total.astype(out.dtype)
    sends(mine, lambda copy: copy.wait_send())
    sends(1 - mine, lambda copy: copy.wait_send())


def solution(mesh):
    n_out, n_inp = mesh.shape["out"], mesh.shape["inp"]
    nx = len({device.coords[0] for device in mesh.devices[:, 0]})

    def local(tensor, state):
        rows_out, rows_inp, width = tensor.shape
        cells_own = state.shape[0]
        cells = n_out * cells_own
        per_owner = n_out // n_inp
        nz = n_out // nx
        group = min(GROUP, rows_out // 4)
        slots = min(SLOTS, rows_out // group - LAST)
        return pl.pallas_call(
            functools.partial(kernel, nx, n_out, n_inp),
            out_shape=pltpu.VMEM((cells // n_inp, rows_out), jnp.bfloat16),
            in_specs=[pl.BlockSpec(memory_space=pl.ANY), pl.BlockSpec(memory_space=pl.ANY)],
            out_specs=pl.BlockSpec(memory_space=pltpu.VMEM),
            scratch_shapes=[
                pltpu.VMEM((cells, width), jnp.bfloat16),
                pltpu.VMEM((cells, rows_inp), jnp.float32),
                pltpu.VMEM((slots, group, rows_inp, width), jnp.bfloat16),
                pltpu.VMEM((cells, rows_out), jnp.float32),
                pltpu.VMEM((n_inp - 1, per_owner, cells_own, rows_out), jnp.float32),
                pltpu.SemaphoreType.DMA,
                pltpu.SemaphoreType.DMA((2, nz)),
                pltpu.SemaphoreType.DMA((2, nx, nz)),
                pltpu.SemaphoreType.DMA((2, nx, nz)),
                pltpu.SemaphoreType.DMA((slots,)),
                pltpu.SemaphoreType.DMA((n_inp - 1, per_owner)),
                pltpu.SemaphoreType.DMA((n_inp - 1, per_owner)),
            ],
            compiler_params=pltpu.CompilerParams(
                collective_id=0, has_side_effects=True, vmem_limit_bytes=60 * 2**20),
            name="collide",
        )(tensor, state)

    return jax.shard_map(
        local, mesh=mesh, in_specs=(P("out", "inp", None), P("out", None)),
        out_specs=P("inp", "out"), check_vma=False)
```

```python
import functools

import jax
import jax.numpy as jnp
from jax import lax
from jax.experimental import pallas as pl
from jax.experimental.pallas import tpu as pltpu
from jax.sharding import PartitionSpec as P

MESH = pl.DeviceIdType.MESH
GROUP = 16
SLOTS = 6
LAST = 2
OWN = 2
NEAR = 3
HOOKS = (8, 10, 16, 24, 32, 48)
ROWS = (((1,), (1,)), ((), ()))


def flip(value, bits):
    for bit in (1 << n for n in range(bits.bit_length())):
        if bits & bit:
            value = value + bit * (1 - 2 * ((value // bit) % 2))
    return value


def differ(a, b, size):
    total = 0
    for bit in (1 << n for n in range((size - 1).bit_length())):
        total = total + bit * ((a // bit + b // bit) % 2)
    return total


def kernel(nx, n_out, n_inp, tensor, state, out, gathered, chosen, slab, parts, landed,
           own_sem, z_sems, x_sems, core_sems, t_sems, s_sems, r_sems):
    rows_out, rows_inp, width = tensor.shape
    cells_own = state.shape[0]
    cells = n_out * cells_own
    nz = n_out // nx
    per_owner = n_out // n_inp
    slots, group = slab.shape[0], slab.shape[1]
    blocks = rows_out // group
    own = min(OWN, slots - 1)
    near = min(NEAR, n_out)
    halves = 2
    half_width = width // halves

    me_o = lax.axis_index("out")
    me_p = lax.axis_index("inp")
    z, x = me_o // nx, me_o % nx
    half = me_p % halves
    partner = me_p + 1 - 2 * half
    cols = pl.ds(pl.multiple_of(half * half_width, 128), half_width)

    def fetch(b, slot):
        return pltpu.make_async_copy(
            tensor.at[pl.ds(b * group, group)], slab.at[slot], t_sems.at[slot])

    own_copy = pltpu.make_async_copy(state, gathered.at[pl.ds(0, cells_own)], own_sem)
    own_copy.start()
    fetch(0, 0).start()

    def out_of(d, e):
        return flip(z, d) * nx + flip(x, e)

    barrier = pltpu.get_barrier_semaphore()
    peers = [(out_of(d, 0), me_p) for d in range(1, nz)]
    peers += [(out_of(0, e), me_p) for e in range(1, nx)]
    peers += [(me_o, lax.rem(me_p + q, n_inp)) for q in range(1, n_inp)]
    for device in peers:
        pl.semaphore_signal(barrier, inc=1, device_id=device, device_id_type=MESH)

    def remote(src, dst, send, recv, device):
        return pltpu.make_async_remote_copy(
            src_ref=src, dst_ref=dst, send_sem=send, recv_sem=recv,
            device_id=device, device_id_type=MESH)

    def shard(d, e):
        return gathered.at[pl.ds((d * nx + e) * cells_own, cells_own), cols]

    def z_copy(d):
        return remote(state.at[:, cols], shard(d, 0), z_sems.at[0, d], z_sems.at[1, d],
                      (out_of(d, 0), me_p))

    def x_copy(e, d):
        return remote(state.at[:, cols] if d == 0 else shard(d, 0), shard(d, e),
                      x_sems.at[0, e, d], x_sems.at[1, e, d], (out_of(0, e), me_p))

    def core_copy(e, d):
        return remote(shard(d, e), shard(d, e), core_sems.at[0, e, d], core_sems.at[1, e, d],
                      (me_o, partner))

    def relay_x(d):
        for e in range(1, nx):
            x_copy(e, d).wait_recv()
            core_copy(e, d).start()

    def relay_z(d):
        z_copy(d).wait_recv()
        for e in range(1, nx):
            x_copy(e, d).start()
        core_copy(0, d).start()

    wide = max(rows_inp, 128)
    first = pl.multiple_of(me_p * rows_inp // wide * wide, wide)

    def choose(start, stop):
        block = gathered[start:stop, pl.ds(first, wide)].astype(jnp.float32)
        piece = block[:, 0:rows_inp]
        for n in range(1, wide // rows_inp):
            piece = jnp.where(me_p % (wide // rows_inp) == n,
                              block[:, n * rows_inp:(n + 1) * rows_inp], piece)
        chosen[start:stop, :] = piece

    def visit(b, slot, start, size, hooks=()):
        rows = pl.ds(start, size)
        lane = lax.broadcasted_iota(jnp.int32, (size, rows_out), 1)
        kept = parts[rows, :]
        for k in range(group):
            for at, act in hooks:
                if at * group // 16 == k:
                    act()
            inner = lax.dot_general(gathered[rows, :], slab[slot, k], ROWS,
                                    preferred_element_type=jnp.float32)
            sums = jnp.sum(inner * chosen[rows, :], axis=1, keepdims=True)
            kept = jnp.where(lane == b * group + k, sums, kept)
        parts[rows, :] = kept

    parts[...] = jnp.zeros_like(parts)
    own_copy.wait()
    choose(0, cells_own)
    pl.semaphore_wait(barrier, len(peers))
    for e in range(1, nx):
        x_copy(e, 0).start()
    for d in range(1, nz):
        z_copy(d).start()
    fetch(1, 1).start()

    hooks = [[] for _ in range(slots)]

    def hook(b, at, act):
        hooks[min(b, slots - 1)].append((at, act))

    hook(own - 1, HOOKS[0], lambda: (relay_x(0), relay_z(1)))
    for d in range(2, nz):
        place = HOOKS[min(2 * d - 3, 3)]
        hook(own + place // 16, place % 16, lambda d=d: relay_z(d))
        place = HOOKS[min(2 * d - 2, 4)]
        hook(own + place // 16, place % 16, lambda d=d: relay_x(d - 1))
    hook(own + HOOKS[5] // 16, HOOKS[5] % 16, lambda: relay_x(nz - 1))

    order = [(d, e) for d in range(nz) for e in range(nx)]
    for b in range(slots):
        if b == own:
            for d, e in order[1:near]:
                core_copy(e, d).wait_recv()
            choose(cells_own, near * cells_own)
        fetch(b, b).wait()
        if b + 2 < slots:
            fetch(b + 2, b + 2).start()
        visit(b, b, 0, (1 if b < own else near) * cells_own, hooks[b])
    for d, e in order[near:]:
        core_copy(e, d).wait_recv()
    choose(near * cells_own, cells)

    def refill(b):
        @pl.when(b + slots < blocks)
        def _():
            fetch(b + slots, b).start()

    def most(b, carry):
        visit(b, b, cells_own, cells - cells_own)
        refill(b)
        return carry

    lax.fori_loop(0, own, most, 0)

    def rest(b, carry):
        visit(b, b, near * cells_own, cells - near * cells_own)
        refill(b)
        return carry

    lax.fori_loop(own, slots, rest, 0)

    count = n_out // 2
    span = count * cells_own
    mine = 1 - differ(z // max(nz // 2, 1), me_p // max(n_inp // 2, 1), 2)
    last = blocks - slots

    def sends(side, act):
        for s in range(count):
            zone = flip(z, s // nx)
            zone = zone + side * (nz // 2) * (1 - 2 * ((zone // (nz // 2)) % 2))
            target = zone * nx + flip(x, s % nx)
            owner, place = target // per_owner, target % per_owner

            @pl.when(owner != me_p)
            def _():
                q = lax.rem(owner - me_p + n_inp, n_inp)
                act(remote(
                    parts.at[pl.ds(pl.multiple_of(side * span, 32) + s * cells_own, cells_own)],
                    landed.at[q - 1, place], s_sems.at[q - 1, place], r_sems.at[q - 1, place],
                    (me_o, owner)))

    def finish(t, carry):
        side = differ(t // last, mine, 2)
        b = slots + t % last

        @pl.when(t < last)
        def _():
            fetch(b, b - slots).wait()

        @pl.when(t == last)
        def _():
            sends(mine, lambda copy: copy.start())

        visit(b, b - slots, pl.multiple_of(side * span, 32), span)
        return carry

    lax.fori_loop(0, 2 * last, finish, 0)
    sends(1 - mine, lambda copy: copy.start())

    for d in range(1, nz):
        z_copy(d).wait_send()
    for d, e in order:
        if e > 0:
            x_copy(e, d).wait_send()
        if (d, e) != (0, 0):
            core_copy(e, d).wait_send()
    for s in range(per_owner):
        target = me_p * per_owner + s
        slot = differ(z, target // nx, nz) * nx + differ(x, target % nx, nx)
        total = parts[pl.ds(pl.multiple_of(slot * cells_own, cells_own), cells_own), :]
        for q in range(1, n_inp):
            remote(landed.at[q - 1, s], landed.at[q - 1, s], s_sems.at[q - 1, s],
                   r_sems.at[q - 1, s], (me_o, partner)).wait_recv()
            total = total + landed[q - 1, s]
        out[s * cells_own:(s + 1) * cells_own, :] = total.astype(out.dtype)
    sends(mine, lambda copy: copy.wait_send())
    sends(1 - mine, lambda copy: copy.wait_send())


def solution(mesh):
    n_out, n_inp = mesh.shape["out"], mesh.shape["inp"]
    nx = len({device.coords[0] for device in mesh.devices[:, 0]})

    def local(tensor, state):
        rows_out, rows_inp, width = tensor.shape
        cells_own = state.shape[0]
        cells = n_out * cells_own
        per_owner = n_out // n_inp
        nz = n_out // nx
        group = min(GROUP, rows_out // 4)
        slots = min(SLOTS, rows_out // group - LAST)
        return pl.pallas_call(
            functools.partial(kernel, nx, n_out, n_inp),
            out_shape=pltpu.VMEM((cells // n_inp, rows_out), jnp.bfloat16),
            in_specs=[pl.BlockSpec(memory_space=pl.ANY), pl.BlockSpec(memory_space=pl.ANY)],
            out_specs=pl.BlockSpec(memory_space=pltpu.VMEM),
            scratch_shapes=[
                pltpu.VMEM((cells, width), jnp.bfloat16),
                pltpu.VMEM((cells, rows_inp), jnp.float32),
                pltpu.VMEM((slots, group, rows_inp, width), jnp.bfloat16),
                pltpu.VMEM((cells, rows_out), jnp.float32),
                pltpu.VMEM((n_inp - 1, per_owner, cells_own, rows_out), jnp.float32),
                pltpu.SemaphoreType.DMA,
                pltpu.SemaphoreType.DMA((2, nz)),
                pltpu.SemaphoreType.DMA((2, nx, nz)),
                pltpu.SemaphoreType.DMA((2, nx, nz)),
                pltpu.SemaphoreType.DMA((slots,)),
                pltpu.SemaphoreType.DMA((n_inp - 1, per_owner)),
                pltpu.SemaphoreType.DMA((n_inp - 1, per_owner)),
            ],
            compiler_params=pltpu.CompilerParams(
                collective_id=0, has_side_effects=True, vmem_limit_bytes=60 * 2**20),
            name="collide",
        )(tensor, state)

    return jax.shard_map(
        local, mesh=mesh, in_specs=(P("out", "inp", None), P("out", None)),
        out_specs=P("inp", "out"), check_vma=False)
```

```python
import functools

import jax
import jax.numpy as jnp
from jax import lax
from jax.experimental import pallas as pl
from jax.experimental.pallas import tpu as pltpu
from jax.sharding import PartitionSpec as P

MESH = pl.DeviceIdType.MESH
GROUP = 16
SLOTS = 6
LAST = 2
OWN = 2
NEAR = 3
HOOKS = (8, 10, 16, 24, 32, 48)
ROWS = (((1,), (1,)), ((), ()))


def flip(value, bits):
    for bit in (1 << n for n in range(bits.bit_length())):
        if bits & bit:
            value = value + bit * (1 - 2 * ((value // bit) % 2))
    return value


def differ(a, b, size):
    total = 0
    for bit in (1 << n for n in range((size - 1).bit_length())):
        total = total + bit * ((a // bit + b // bit) % 2)
    return total


def kernel(nx, n_out, n_inp, tensor, state, out, gathered, chosen, slab, parts, landed,
           own_sem, z_sems, x_sems, core_sems, t_sems, s_sems, r_sems):
    rows_out, rows_inp, width = tensor.shape
    cells_own = state.shape[0]
    cells = n_out * cells_own
    nz = n_out // nx
    per_owner = n_out // n_inp
    slots, group = slab.shape[0], slab.shape[1]
    blocks = rows_out // group
    own = min(OWN, slots - 1)
    near = min(NEAR, n_out)
    halves = 2
    half_width = width // halves

    me_o = lax.axis_index("out")
    me_p = lax.axis_index("inp")
    z, x = me_o // nx, me_o % nx
    half = me_p % halves
    partner = me_p + 1 - 2 * half
    cols = pl.ds(pl.multiple_of(half * half_width, 128), half_width)

    def fetch(b, slot):
        return pltpu.make_async_copy(
            tensor.at[pl.ds(b * group, group)], slab.at[slot], t_sems.at[slot])

    own_copy = pltpu.make_async_copy(state, gathered.at[pl.ds(0, cells_own)], own_sem)
    own_copy.start()
    fetch(0, 0).start()

    def out_of(d, e):
        return flip(z, d) * nx + flip(x, e)

    barrier = pltpu.get_barrier_semaphore()
    peers = [(out_of(d, 0), me_p) for d in range(1, nz)]
    peers += [(out_of(0, e), me_p) for e in range(1, nx)]
    peers += [(me_o, lax.rem(me_p + q, n_inp)) for q in range(1, n_inp)]
    for device in peers:
        pl.semaphore_signal(barrier, inc=1, device_id=device, device_id_type=MESH)

    def remote(src, dst, send, recv, device):
        return pltpu.make_async_remote_copy(
            src_ref=src, dst_ref=dst, send_sem=send, recv_sem=recv,
            device_id=device, device_id_type=MESH)

    def shard(d, e):
        return gathered.at[pl.ds((d * nx + e) * cells_own, cells_own), cols]

    def z_copy(d):
        return remote(state.at[:, cols], shard(d, 0), z_sems.at[0, d], z_sems.at[1, d],
                      (out_of(d, 0), me_p))

    def x_copy(e, d):
        return remote(state.at[:, cols] if d == 0 else shard(d, 0), shard(d, e),
                      x_sems.at[0, e, d], x_sems.at[1, e, d], (out_of(0, e), me_p))

    def core_copy(e, d):
        return remote(shard(d, e), shard(d, e), core_sems.at[0, e, d], core_sems.at[1, e, d],
                      (me_o, partner))

    def relay_x(d):
        for e in range(1, nx):
            x_copy(e, d).wait_recv()
            core_copy(e, d).start()

    def relay_z(d):
        z_copy(d).wait_recv()
        for e in range(1, nx):
            x_copy(e, d).start()
        core_copy(0, d).start()

    wide = max(rows_inp, 128)
    first = pl.multiple_of(me_p * rows_inp // wide * wide, wide)

    def choose(start, stop):
        block = gathered[start:stop, pl.ds(first, wide)].astype(jnp.float32)
        piece = block[:, 0:rows_inp]
        for n in range(1, wide // rows_inp):
            piece = jnp.where(me_p % (wide // rows_inp) == n,
                              block[:, n * rows_inp:(n + 1) * rows_inp], piece)
        chosen[start:stop, :] = piece

    def visit(b, slot, start, size, hooks=()):
        rows = pl.ds(start, size)
        lane = lax.broadcasted_iota(jnp.int32, (size, rows_out), 1)
        kept = parts[rows, :]
        for k in range(group):
            for at, act in hooks:
                if at * group // 16 == k:
                    act()
            inner = lax.dot_general(gathered[rows, :], slab[slot, k], ROWS,
                                    preferred_element_type=jnp.float32)
            sums = jnp.sum(inner * chosen[rows, :], axis=1, keepdims=True)
            kept = jnp.where(lane == b * group + k, sums, kept)
        parts[rows, :] = kept

    parts[...] = jnp.zeros_like(parts)
    own_copy.wait()
    choose(0, cells_own)
    pl.semaphore_wait(barrier, len(peers))
    for e in range(1, nx):
        x_copy(e, 0).start()
    for d in range(1, nz):
        z_copy(d).start()
    fetch(1, 1).start()

    hooks = [[] for _ in range(slots)]

    def hook(b, at, act):
        hooks[min(b, slots - 1)].append((at, act))

    hook(own - 1, HOOKS[0], lambda: (relay_x(0), relay_z(1)))
    for d in range(2, nz):
        place = HOOKS[min(2 * d - 3, 3)]
        hook(own + place // 16, place % 16, lambda d=d: relay_z(d))
        place = HOOKS[min(2 * d - 2, 4)]
        hook(own + place // 16, place % 16, lambda d=d: relay_x(d - 1))
    hook(own + HOOKS[5] // 16, HOOKS[5] % 16, lambda: relay_x(nz - 1))

    order = [(d, e) for d in range(nz) for e in range(nx)]
    for b in range(slots):
        if b == own:
            for d, e in order[1:near]:
                core_copy(e, d).wait_recv()
            choose(cells_own, near * cells_own)
        fetch(b, b).wait()
        if b + 2 < slots:
            fetch(b + 2, b + 2).start()
        visit(b, b, 0, (1 if b < own else near) * cells_own, hooks[b])
    for d, e in order[near:]:
        core_copy(e, d).wait_recv()
    choose(near * cells_own, cells)

    def refill(b):
        @pl.when(b + slots < blocks)
        def _():
            fetch(b + slots, b).start()

    def most(b, carry):
        visit(b, b, cells_own, cells - cells_own)
        refill(b)
        return carry

    lax.fori_loop(0, own, most, 0)

    pair = 2 if (slots - own) % 2 == 0 else 1

    def rest(i, carry):
        for n in range(pair):
            b = own + i * pair + n
            visit(b, b, near * cells_own, cells - near * cells_own)
        for n in range(pair):
            refill(own + i * pair + n)
        return carry

    lax.fori_loop(0, (slots - own) // pair, rest, 0)

    count = n_out // 2
    span = count * cells_own
    mine = 1 - differ(z // max(nz // 2, 1), me_p // max(n_inp // 2, 1), 2)

    def sends(side, act):
        for s in range(count):
            zone = flip(z, s // nx)
            zone = zone + side * (nz // 2) * (1 - 2 * ((zone // (nz // 2)) % 2))
            target = zone * nx + flip(x, s % nx)
            owner, place = target // per_owner, target % per_owner

            @pl.when(owner != me_p)
            def _():
                q = lax.rem(owner - me_p + n_inp, n_inp)
                act(remote(
                    parts.at[pl.ds(pl.multiple_of(side * span, 32) + s * cells_own, cells_own)],
                    landed.at[q - 1, place], s_sems.at[q - 1, place], r_sems.at[q - 1, place],
                    (me_o, owner)))

    def finish(t, carry):
        side = differ(t, mine, 2)

        @pl.when(t == 1)
        def _():
            sends(mine, lambda copy: copy.start())

        for b in range(slots, blocks):
            visit(b, b - slots, pl.multiple_of(side * span, 32), span)
        return carry

    for b in range(slots, blocks):
        fetch(b, b - slots).wait()
    lax.fori_loop(0, 2, finish, 0)
    sends(1 - mine, lambda copy: copy.start())

    for d in range(1, nz):
        z_copy(d).wait_send()
    for d, e in order:
        if e > 0:
            x_copy(e, d).wait_send()
        if (d, e) != (0, 0):
            core_copy(e, d).wait_send()
    for s in range(per_owner):
        target = me_p * per_owner + s
        slot = differ(z, target // nx, nz) * nx + differ(x, target % nx, nx)
        total = parts[pl.ds(pl.multiple_of(slot * cells_own, cells_own), cells_own), :]
        for q in range(1, n_inp):
            remote(landed.at[q - 1, s], landed.at[q - 1, s], s_sems.at[q - 1, s],
                   r_sems.at[q - 1, s], (me_o, partner)).wait_recv()
            total = total + landed[q - 1, s]
        out[s * cells_own:(s + 1) * cells_own, :] = total.astype(out.dtype)
    sends(mine, lambda copy: copy.wait_send())
    sends(1 - mine, lambda copy: copy.wait_send())


def solution(mesh):
    n_out, n_inp = mesh.shape["out"], mesh.shape["inp"]
    nx = len({device.coords[0] for device in mesh.devices[:, 0]})

    def local(tensor, state):
        rows_out, rows_inp, width = tensor.shape
        cells_own = state.shape[0]
        cells = n_out * cells_own
        per_owner = n_out // n_inp
        nz = n_out // nx
        group = min(GROUP, rows_out // 4)
        slots = min(SLOTS, rows_out // group - LAST)
        return pl.pallas_call(
            functools.partial(kernel, nx, n_out, n_inp),
            out_shape=pltpu.VMEM((cells // n_inp, rows_out), jnp.bfloat16),
            in_specs=[pl.BlockSpec(memory_space=pl.ANY), pl.BlockSpec(memory_space=pl.ANY)],
            out_specs=pl.BlockSpec(memory_space=pltpu.VMEM),
            scratch_shapes=[
                pltpu.VMEM((cells, width), jnp.bfloat16),
                pltpu.VMEM((cells, rows_inp), jnp.float32),
                pltpu.VMEM((slots, group, rows_inp, width), jnp.bfloat16),
                pltpu.VMEM((cells, rows_out), jnp.float32),
                pltpu.VMEM((n_inp - 1, per_owner, cells_own, rows_out), jnp.float32),
                pltpu.SemaphoreType.DMA,
                pltpu.SemaphoreType.DMA((2, nz)),
                pltpu.SemaphoreType.DMA((2, nx, nz)),
                pltpu.SemaphoreType.DMA((2, nx, nz)),
                pltpu.SemaphoreType.DMA((slots,)),
                pltpu.SemaphoreType.DMA((n_inp - 1, per_owner)),
                pltpu.SemaphoreType.DMA((n_inp - 1, per_owner)),
            ],
            compiler_params=pltpu.CompilerParams(
                collective_id=0, has_side_effects=True, vmem_limit_bytes=60 * 2**20),
            name="collide",
        )(tensor, state)

    return jax.shard_map(
        local, mesh=mesh, in_specs=(P("out", "inp", None), P("out", None)),
        out_specs=P("inp", "out"), check_vma=False)
```

```python
import functools

import jax
import jax.numpy as jnp
from jax import lax
from jax.experimental import pallas as pl
from jax.experimental.pallas import tpu as pltpu
from jax.sharding import PartitionSpec as P

MESH = pl.DeviceIdType.MESH
GROUP = 16
SLOTS = 6
LAST = 2
OWN = 2
NEAR = 3
HOOKS = (8, 10, 16, 24, 32, 48)
ROWS = (((1,), (1,)), ((), ()))


def flip(value, bits):
    for bit in (1 << n for n in range(bits.bit_length())):
        if bits & bit:
            value = value + bit * (1 - 2 * ((value // bit) % 2))
    return value


def differ(a, b, size):
    total = 0
    for bit in (1 << n for n in range((size - 1).bit_length())):
        total = total + bit * ((a // bit + b // bit) % 2)
    return total


def kernel(nx, n_out, n_inp, tensor, state, out, gathered, chosen, slab, parts, landed,
           own_sem, z_sems, x_sems, core_sems, t_sems, s_sems, r_sems):
    rows_out, rows_inp, width = tensor.shape
    cells_own = state.shape[0]
    cells = n_out * cells_own
    nz = n_out // nx
    per_owner = n_out // n_inp
    slots, group = slab.shape[0], slab.shape[1]
    blocks = rows_out // group
    own = min(OWN, slots - 1)
    near = min(NEAR, n_out)
    halves = 2
    half_width = width // halves

    me_o = lax.axis_index("out")
    me_p = lax.axis_index("inp")
    z, x = me_o // nx, me_o % nx
    half = me_p % halves
    partner = me_p + 1 - 2 * half
    cols = pl.ds(pl.multiple_of(half * half_width, 128), half_width)

    def fetch(b, slot):
        return pltpu.make_async_copy(
            tensor.at[pl.ds(b * group, group)], slab.at[slot], t_sems.at[slot])

    own_copy = pltpu.make_async_copy(state, gathered.at[pl.ds(0, cells_own)], own_sem)
    own_copy.start()
    fetch(0, 0).start()

    def out_of(d, e):
        return flip(z, d) * nx + flip(x, e)

    barrier = pltpu.get_barrier_semaphore()
    peers = [(out_of(d, 0), me_p) for d in range(1, nz)]
    peers += [(out_of(0, e), me_p) for e in range(1, nx)]
    peers += [(me_o, lax.rem(me_p + q, n_inp)) for q in range(1, n_inp)]
    for device in peers:
        pl.semaphore_signal(barrier, inc=1, device_id=device, device_id_type=MESH)

    def remote(src, dst, send, recv, device):
        return pltpu.make_async_remote_copy(
            src_ref=src, dst_ref=dst, send_sem=send, recv_sem=recv,
            device_id=device, device_id_type=MESH)

    def shard(d, e):
        return gathered.at[pl.ds((d * nx + e) * cells_own, cells_own), cols]

    def z_copy(d):
        return remote(state.at[:, cols], shard(d, 0), z_sems.at[0, d], z_sems.at[1, d],
                      (out_of(d, 0), me_p))

    def x_copy(e, d):
        return remote(state.at[:, cols] if d == 0 else shard(d, 0), shard(d, e),
                      x_sems.at[0, e, d], x_sems.at[1, e, d], (out_of(0, e), me_p))

    def core_copy(e, d):
        return remote(shard(d, e), shard(d, e), core_sems.at[0, e, d], core_sems.at[1, e, d],
                      (me_o, partner))

    def relay_x(d):
        for e in range(1, nx):
            x_copy(e, d).wait_recv()
            core_copy(e, d).start()

    def relay_z(d):
        z_copy(d).wait_recv()
        for e in range(1, nx):
            x_copy(e, d).start()
        core_copy(0, d).start()

    wide = max(rows_inp, 128)
    first = pl.multiple_of(me_p * rows_inp // wide * wide, wide)

    def choose(start, stop):
        block = gathered[start:stop, pl.ds(first, wide)].astype(jnp.float32)
        piece = block[:, 0:rows_inp]
        for n in range(1, wide // rows_inp):
            piece = jnp.where(me_p % (wide // rows_inp) == n,
                              block[:, n * rows_inp:(n + 1) * rows_inp], piece)
        chosen[start:stop, :] = piece

    def visit(b, slot, start, size, hooks=()):
        rows = pl.ds(start, size)
        lane = lax.broadcasted_iota(jnp.int32, (size, rows_out), 1)
        kept = parts[rows, :]
        for k in range(group):
            for at, act in hooks:
                if at * group // 16 == k:
                    act()
            inner = lax.dot_general(gathered[rows, :], slab[slot, k], ROWS,
                                    preferred_element_type=jnp.float32)
            sums = jnp.sum(inner * chosen[rows, :], axis=1, keepdims=True)
            kept = jnp.where(lane == b * group + k, sums, kept)
        parts[rows, :] = kept

    parts[...] = jnp.zeros_like(parts)
    pl.semaphore_wait(barrier, len(peers))
    for e in range(1, nx):
        x_copy(e, 0).start()
    for d in range(1, nz):
        z_copy(d).start()
    fetch(1, 1).start()
    own_copy.wait()
    choose(0, cells_own)

    hooks = [[] for _ in range(slots)]

    def hook(b, at, act):
        hooks[min(b, slots - 1)].append((at, act))

    hook(own - 1, HOOKS[0], lambda: (relay_x(0), relay_z(1)))
    for d in range(2, nz):
        place = HOOKS[min(2 * d - 3, 3)]
        hook(own + place // 16, place % 16, lambda d=d: relay_z(d))
        place = HOOKS[min(2 * d - 2, 4)]
        hook(own + place // 16, place % 16, lambda d=d: relay_x(d - 1))
    hook(own + HOOKS[5] // 16, HOOKS[5] % 16, lambda: relay_x(nz - 1))

    order = [(d, e) for d in range(nz) for e in range(nx)]
    for b in range(slots):
        if b == own:
            for d, e in order[1:near]:
                core_copy(e, d).wait_recv()
            choose(cells_own, near * cells_own)
        fetch(b, b).wait()
        if b + 2 < slots:
            fetch(b + 2, b + 2).start()
        visit(b, b, 0, (1 if b < own else near) * cells_own, hooks[b])
    for d, e in order[near:]:
        core_copy(e, d).wait_recv()
    choose(near * cells_own, cells)

    def refill(b):
        @pl.when(b + slots < blocks)
        def _():
            fetch(b + slots, b).start()

    def most(b, carry):
        visit(b, b, cells_own, cells - cells_own)
        refill(b)
        return carry

    lax.fori_loop(0, own, most, 0)

    pair = 2 if (slots - own) % 2 == 0 else 1

    def rest(i, carry):
        for n in range(pair):
            b = own + i * pair + n
            visit(b, b, near * cells_own, cells - near * cells_own)
        for n in range(pair):
            refill(own + i * pair + n)
        return carry

    lax.fori_loop(0, (slots - own) // pair, rest, 0)

    count = n_out // 2
    span = count * cells_own
    mine = 1 - differ(z // max(nz // 2, 1), me_p // max(n_inp // 2, 1), 2)

    def sends(side, act):
        for s in range(count):
            zone = flip(z, s // nx)
            zone = zone + side * (nz // 2) * (1 - 2 * ((zone // (nz // 2)) % 2))
            target = zone * nx + flip(x, s % nx)
            owner, place = target // per_owner, target % per_owner

            @pl.when(owner != me_p)
            def _():
                q = lax.rem(owner - me_p + n_inp, n_inp)
                act(remote(
                    parts.at[pl.ds(pl.multiple_of(side * span, 32) + s * cells_own, cells_own)],
                    landed.at[q - 1, place], s_sems.at[q - 1, place], r_sems.at[q - 1, place],
                    (me_o, owner)))

    def finish(t, carry):
        side = differ(t, mine, 2)

        @pl.when(t == 1)
        def _():
            sends(mine, lambda copy: copy.start())

        for b in range(slots, blocks):
            visit(b, b - slots, pl.multiple_of(side * span, 32), span)
        return carry

    for b in range(slots, blocks):
        fetch(b, b - slots).wait()
    lax.fori_loop(0, 2, finish, 0)
    sends(1 - mine, lambda copy: copy.start())

    for d in range(1, nz):
        z_copy(d).wait_send()
    for d, e in order:
        if e > 0:
            x_copy(e, d).wait_send()
        if (d, e) != (0, 0):
            core_copy(e, d).wait_send()
    for s in range(per_owner):
        target = me_p * per_owner + s
        slot = differ(z, target // nx, nz) * nx + differ(x, target % nx, nx)
        total = parts[pl.ds(pl.multiple_of(slot * cells_own, cells_own), cells_own), :]
        for q in range(1, n_inp):
            remote(landed.at[q - 1, s], landed.at[q - 1, s], s_sems.at[q - 1, s],
                   r_sems.at[q - 1, s], (me_o, partner)).wait_recv()
            total = total + landed[q - 1, s]
        out[s * cells_own:(s + 1) * cells_own, :] = total.astype(out.dtype)
    sends(mine, lambda copy: copy.wait_send())
    sends(1 - mine, lambda copy: copy.wait_send())


def solution(mesh):
    n_out, n_inp = mesh.shape["out"], mesh.shape["inp"]
    nx = len({device.coords[0] for device in mesh.devices[:, 0]})

    def local(tensor, state):
        rows_out, rows_inp, width = tensor.shape
        cells_own = state.shape[0]
        cells = n_out * cells_own
        per_owner = n_out // n_inp
        nz = n_out // nx
        group = min(GROUP, rows_out // 4)
        slots = min(SLOTS, rows_out // group - LAST)
        return pl.pallas_call(
            functools.partial(kernel, nx, n_out, n_inp),
            out_shape=pltpu.VMEM((cells // n_inp, rows_out), jnp.bfloat16),
            in_specs=[pl.BlockSpec(memory_space=pl.ANY), pl.BlockSpec(memory_space=pl.ANY)],
            out_specs=pl.BlockSpec(memory_space=pltpu.VMEM),
            scratch_shapes=[
                pltpu.VMEM((cells, width), jnp.bfloat16),
                pltpu.VMEM((cells, rows_inp), jnp.float32),
                pltpu.VMEM((slots, group, rows_inp, width), jnp.bfloat16),
                pltpu.VMEM((cells, rows_out), jnp.float32),
                pltpu.VMEM((n_inp - 1, per_owner, cells_own, rows_out), jnp.float32),
                pltpu.SemaphoreType.DMA,
                pltpu.SemaphoreType.DMA((2, nz)),
                pltpu.SemaphoreType.DMA((2, nx, nz)),
                pltpu.SemaphoreType.DMA((2, nx, nz)),
                pltpu.SemaphoreType.DMA((slots,)),
                pltpu.SemaphoreType.DMA((n_inp - 1, per_owner)),
                pltpu.SemaphoreType.DMA((n_inp - 1, per_owner)),
            ],
            compiler_params=pltpu.CompilerParams(
                collective_id=0, has_side_effects=True, vmem_limit_bytes=60 * 2**20),
            name="collide",
        )(tensor, state)

    return jax.shard_map(
        local, mesh=mesh, in_specs=(P("out", "inp", None), P("out", None)),
        out_specs=P("inp", "out"), check_vma=False)
```

```python
import functools

import jax
import jax.numpy as jnp
from jax import lax
from jax.experimental import pallas as pl
from jax.experimental.pallas import tpu as pltpu
from jax.sharding import PartitionSpec as P

MESH = pl.DeviceIdType.MESH
GROUP = 16
SLOTS = 6
LAST = 2
OWN = 2
NEAR = 3
HOOKS = (8, 9, 15, 24, 30, 46)
ROWS = (((1,), (1,)), ((), ()))


def flip(value, bits):
    for bit in (1 << n for n in range(bits.bit_length())):
        if bits & bit:
            value = value + bit * (1 - 2 * ((value // bit) % 2))
    return value


def differ(a, b, size):
    total = 0
    for bit in (1 << n for n in range((size - 1).bit_length())):
        total = total + bit * ((a // bit + b // bit) % 2)
    return total


def kernel(nx, n_out, n_inp, tensor, state, out, gathered, chosen, slab, parts, landed,
           own_sem, z_sems, x_sems, core_sems, t_sems, s_sems, r_sems):
    rows_out, rows_inp, width = tensor.shape
    cells_own = state.shape[0]
    cells = n_out * cells_own
    nz = n_out // nx
    per_owner = n_out // n_inp
    slots, group = slab.shape[0], slab.shape[1]
    blocks = rows_out // group
    own = min(OWN, slots - 1)
    near = min(NEAR, n_out)
    halves = 2
    half_width = width // halves

    me_o = lax.axis_index("out")
    me_p = lax.axis_index("inp")
    z, x = me_o // nx, me_o % nx
    half = me_p % halves
    partner = me_p + 1 - 2 * half
    cols = pl.ds(pl.multiple_of(half * half_width, 128), half_width)

    def fetch(b, slot):
        return pltpu.make_async_copy(
            tensor.at[pl.ds(b * group, group)], slab.at[slot], t_sems.at[slot])

    own_copy = pltpu.make_async_copy(state, gathered.at[pl.ds(0, cells_own)], own_sem)
    own_copy.start()
    fetch(0, 0).start()

    def out_of(d, e):
        return flip(z, d) * nx + flip(x, e)

    barrier = pltpu.get_barrier_semaphore()
    peers = [(out_of(d, 0), me_p) for d in range(1, nz)]
    peers += [(out_of(0, e), me_p) for e in range(1, nx)]
    peers += [(me_o, lax.rem(me_p + q, n_inp)) for q in range(1, n_inp)]
    for device in peers:
        pl.semaphore_signal(barrier, inc=1, device_id=device, device_id_type=MESH)

    def remote(src, dst, send, recv, device):
        return pltpu.make_async_remote_copy(
            src_ref=src, dst_ref=dst, send_sem=send, recv_sem=recv,
            device_id=device, device_id_type=MESH)

    def shard(d, e):
        return gathered.at[pl.ds((d * nx + e) * cells_own, cells_own), cols]

    def z_copy(d):
        return remote(state.at[:, cols], shard(d, 0), z_sems.at[0, d], z_sems.at[1, d],
                      (out_of(d, 0), me_p))

    def x_copy(e, d):
        return remote(state.at[:, cols] if d == 0 else shard(d, 0), shard(d, e),
                      x_sems.at[0, e, d], x_sems.at[1, e, d], (out_of(0, e), me_p))

    def core_copy(e, d):
        return remote(shard(d, e), shard(d, e), core_sems.at[0, e, d], core_sems.at[1, e, d],
                      (me_o, partner))

    def relay_x(d):
        for e in range(1, nx):
            x_copy(e, d).wait_recv()
            core_copy(e, d).start()

    def relay_z(d):
        z_copy(d).wait_recv()
        for e in range(1, nx):
            x_copy(e, d).start()
        core_copy(0, d).start()

    wide = max(rows_inp, 128)
    first = pl.multiple_of(me_p * rows_inp // wide * wide, wide)

    def choose(start, stop):
        block = gathered[start:stop, pl.ds(first, wide)].astype(jnp.float32)
        piece = block[:, 0:rows_inp]
        for n in range(1, wide // rows_inp):
            piece = jnp.where(me_p % (wide // rows_inp) == n,
                              block[:, n * rows_inp:(n + 1) * rows_inp], piece)
        chosen[start:stop, :] = piece

    def visit(b, slot, start, size, hooks=()):
        rows = pl.ds(start, size)
        lane = lax.broadcasted_iota(jnp.int32, (size, rows_out), 1)
        kept = parts[rows, :]
        for k in range(group):
            for at, act in hooks:
                if at * group // 16 == k:
                    act()
            inner = lax.dot_general(gathered[rows, :], slab[slot, k], ROWS,
                                    preferred_element_type=jnp.float32)
            sums = jnp.sum(inner * chosen[rows, :], axis=1, keepdims=True)
            kept = jnp.where(lane == b * group + k, sums, kept)
        parts[rows, :] = kept

    parts[...] = jnp.zeros_like(parts)
    pl.semaphore_wait(barrier, len(peers))
    for e in range(1, nx):
        x_copy(e, 0).start()
    for d in range(1, nz):
        z_copy(d).start()
    fetch(1, 1).start()
    own_copy.wait()
    choose(0, cells_own)

    hooks = [[] for _ in range(slots)]

    def hook(b, at, act):
        hooks[min(b, slots - 1)].append((at, act))

    hook(own - 1, HOOKS[0], lambda: (relay_x(0), relay_z(1)))
    for d in range(2, nz):
        place = HOOKS[min(2 * d - 3, 3)]
        hook(own + place // 16, place % 16, lambda d=d: relay_z(d))
        place = HOOKS[min(2 * d - 2, 4)]
        hook(own + place // 16, place % 16, lambda d=d: relay_x(d - 1))
    hook(own + HOOKS[5] // 16, HOOKS[5] % 16, lambda: relay_x(nz - 1))

    order = [(d, e) for d in range(nz) for e in range(nx)]
    for b in range(slots):
        if b == own:
            for d, e in order[1:near]:
                core_copy(e, d).wait_recv()
            choose(cells_own, near * cells_own)
        fetch(b, b).wait()
        if b + 2 < slots:
            fetch(b + 2, b + 2).start()
        visit(b, b, 0, (1 if b < own else near) * cells_own, hooks[b])
    for d, e in order[near:]:
        core_copy(e, d).wait_recv()
    choose(near * cells_own, cells)

    def refill(b):
        @pl.when(b + slots < blocks)
        def _():
            fetch(b + slots, b).start()

    def most(b, carry):
        visit(b, b, cells_own, cells - cells_own)
        refill(b)
        return carry

    lax.fori_loop(0, own, most, 0)

    pair = 2 if (slots - own) % 2 == 0 else 1

    def rest(i, carry):
        for n in range(pair):
            b = own + i * pair + n
            visit(b, b, near * cells_own, cells - near * cells_own)
        for n in range(pair):
            refill(own + i * pair + n)
        return carry

    lax.fori_loop(0, (slots - own) // pair, rest, 0)

    count = n_out // 2
    span = count * cells_own
    mine = 1 - differ(z // max(nz // 2, 1), me_p // max(n_inp // 2, 1), 2)

    def sends(side, act):
        for s in range(count):
            zone = flip(z, s // nx)
            zone = zone + side * (nz // 2) * (1 - 2 * ((zone // (nz // 2)) % 2))
            target = zone * nx + flip(x, s % nx)
            owner, place = target // per_owner, target % per_owner

            @pl.when(owner != me_p)
            def _():
                q = lax.rem(owner - me_p + n_inp, n_inp)
                act(remote(
                    parts.at[pl.ds(pl.multiple_of(side * span, 32) + s * cells_own, cells_own)],
                    landed.at[q - 1, place], s_sems.at[q - 1, place], r_sems.at[q - 1, place],
                    (me_o, owner)))

    def finish(t, carry):
        side = differ(t, mine, 2)

        @pl.when(t == 1)
        def _():
            sends(mine, lambda copy: copy.start())

        for b in range(slots, blocks):
            visit(b, b - slots, pl.multiple_of(side * span, 32), span)
        return carry

    for b in range(slots, blocks):
        fetch(b, b - slots).wait()
    lax.fori_loop(0, 2, finish, 0)
    sends(1 - mine, lambda copy: copy.start())

    for d in range(1, nz):
        z_copy(d).wait_send()
    for d, e in order:
        if e > 0:
            x_copy(e, d).wait_send()
        if (d, e) != (0, 0):
            core_copy(e, d).wait_send()
    for s in range(per_owner):
        target = me_p * per_owner + s
        slot = differ(z, target // nx, nz) * nx + differ(x, target % nx, nx)
        total = parts[pl.ds(pl.multiple_of(slot * cells_own, cells_own), cells_own), :]
        for q in range(1, n_inp):
            remote(landed.at[q - 1, s], landed.at[q - 1, s], s_sems.at[q - 1, s],
                   r_sems.at[q - 1, s], (me_o, partner)).wait_recv()
            total = total + landed[q - 1, s]
        out[s * cells_own:(s + 1) * cells_own, :] = total.astype(out.dtype)
    sends(mine, lambda copy: copy.wait_send())
    sends(1 - mine, lambda copy: copy.wait_send())


def solution(mesh):
    n_out, n_inp = mesh.shape["out"], mesh.shape["inp"]
    nx = len({device.coords[0] for device in mesh.devices[:, 0]})

    def local(tensor, state):
        rows_out, rows_inp, width = tensor.shape
        cells_own = state.shape[0]
        cells = n_out * cells_own
        per_owner = n_out // n_inp
        nz = n_out // nx
        group = min(GROUP, rows_out // 4)
        slots = min(SLOTS, rows_out // group - LAST)
        return pl.pallas_call(
            functools.partial(kernel, nx, n_out, n_inp),
            out_shape=pltpu.VMEM((cells // n_inp, rows_out), jnp.bfloat16),
            in_specs=[pl.BlockSpec(memory_space=pl.ANY), pl.BlockSpec(memory_space=pl.ANY)],
            out_specs=pl.BlockSpec(memory_space=pltpu.VMEM),
            scratch_shapes=[
                pltpu.VMEM((cells, width), jnp.bfloat16),
                pltpu.VMEM((cells, rows_inp), jnp.float32),
                pltpu.VMEM((slots, group, rows_inp, width), jnp.bfloat16),
                pltpu.VMEM((cells, rows_out), jnp.float32),
                pltpu.VMEM((n_inp - 1, per_owner, cells_own, rows_out), jnp.float32),
                pltpu.SemaphoreType.DMA,
                pltpu.SemaphoreType.DMA((2, nz)),
                pltpu.SemaphoreType.DMA((2, nx, nz)),
                pltpu.SemaphoreType.DMA((2, nx, nz)),
                pltpu.SemaphoreType.DMA((slots,)),
                pltpu.SemaphoreType.DMA((n_inp - 1, per_owner)),
                pltpu.SemaphoreType.DMA((n_inp - 1, per_owner)),
            ],
            compiler_params=pltpu.CompilerParams(
                collective_id=0, has_side_effects=True, vmem_limit_bytes=60 * 2**20),
            name="collide",
        )(tensor, state)

    return jax.shard_map(
        local, mesh=mesh, in_specs=(P("out", "inp", None), P("out", None)),
        out_specs=P("inp", "out"), check_vma=False)
```
